32 devices in a mesh: train: 4 (over y, x), induce: 8 (over z, core).
Axes of the slice: x: 2, y: 2, z: 4, core: 2. Of those that a mesh axis runs over, the one named last changes fastest.
Arguments:
- train_coords: float32 [256, 192], P('train'), may hold values from -0.3 to 4.8, as said below
- induce_coords: float32 [1024, 192], P('induce'), may hold values from -0.3 to 4.8, as said below
- train_forces: float32 [256, 192], P('train'), may hold values from -18 to 18
- atom_pairs: int32 [2, 2016], replicated, may hold values from 0 to 63, as said below
- length_scale: float32 [1], replicated, may hold values from 1.5 to 3
Outputs:
- coefficients: float32 [1024, 192], P('induce')
- residual: float32 [1024, 192], P('induce')
- desc_coeffs: float32 [1024, 2016], P('induce')
The draws below stay inside these ranges and needn't reach their ends.
Inputs may be any that keep to these rules, and one draw needn't show every extreme that they name: `atom_pairs`: every unordered pair of two different atoms of the 64 stands in exactly one column, in either order. `train_coords`: atom a lies within 0.3 of 1.5 * (a % 4, a // 4 % 4, a // 16) in each component. `induce_coords`: atom a lies within 0.3 of 1.5 * (a % 4, a // 4 % 4, a // 16) in each component.
All inputs are finite; a program needn't handle non-finite values.
Results may differ from the reference program's by a relative error of at most 0.0085.
Values sent between devices are 32-bit elements; how exact they have to be, the bound alone decides.
No kernel may reach another device: no remote copies, remote signals or barrier semaphores. Data moves between devices by JAX's collectives and lax.ppermute only.
A program may use at most 64 MiB of HBM per device.

```python
import math
import jax
import jax.numpy as jnp
import numpy as np
from jax import lax

ATOMS = 64
DESC = 2016
COMP = 192
TRAIN_DEV = 64
STEPS = 2
TRAIN_ALL = 256
INDUCE_ALL = 1024
N_TRAIN = 4


def geometry_draw(key, row_count):
    atom_ids = jnp.arange(ATOMS, dtype=jnp.int32)
    lattice = 1.5 * jnp.stack([atom_ids % 4, atom_ids // 4 % 4, atom_ids // 16]).astype(jnp.float32)
    jitter = jax.random.uniform(key, (row_count, 3, ATOMS), jnp.float32, -0.3, 0.3)
    return (lattice[None, :, :] + jitter).reshape(row_count, 3 * ATOMS)


def draw_train_coords(key, part):
    return geometry_draw(jax.random.fold_in(key, 11), TRAIN_ALL)


def draw_induce_coords(key, part):
    return geometry_draw(jax.random.fold_in(key, 23), INDUCE_ALL)


def draw_train_forces(key, part):
    row_pos = jnp.arange(TRAIN_ALL, dtype=jnp.float32) / max(TRAIN_ALL - 1, 1)
    inner_key = jax.random.fold_in(key, 43)
    row_scale = 1.0 + 2.0 * row_pos
    noise = jnp.clip(jax.random.normal(inner_key, (TRAIN_ALL, COMP), jnp.float32), -6.0, 6.0)
    return noise * row_scale[:, None]


def draw_atom_pairs(key, part):
    lower_atom, upper_atom = np.triu_indices(ATOMS, 1)
    shuffled = jax.random.permutation(jax.random.fold_in(key, 31), DESC)
    flipped = jax.random.randint(jax.random.fold_in(key, 37), (DESC,), 0, 2)
    head_atom = jnp.asarray(lower_atom, jnp.int32)[shuffled]
    tail_atom = jnp.asarray(upper_atom, jnp.int32)[shuffled]
    first_row = jnp.where(flipped == 1, tail_atom, head_atom)
    second_row = jnp.where(flipped == 1, head_atom, tail_atom)
    return jnp.stack([first_row, second_row]).astype(jnp.int32)


def setup_inputs(seed: int = 0) -> dict:
    key_of = jax.random.split(jax.random.key(seed), 6)
    train_coords = draw_train_coords(jax.random.fold_in(key_of[5], 71), 0)
    induce_coords = draw_induce_coords(jax.random.fold_in(key_of[5], 71), 0)
    train_forces = draw_train_forces(jax.random.fold_in(key_of[5], 71), 0)
    atom_pairs = draw_atom_pairs(jax.random.fold_in(key_of[5], 71), 0)
    length_scale = jnp.clip(jax.random.uniform(key_of[4], (1,), jnp.float32, 1.5, 3.0), 1.5, 3.0)
    return dict(train_coords=train_coords, induce_coords=induce_coords, train_forces=train_forces, atom_pairs=atom_pairs, length_scale=length_scale)


root_five = math.sqrt(5.0)

def make_incidence(atom_pairs, atom_count):
    atom_ids = jnp.arange(atom_count, dtype=jnp.int32)
    head_hit = (atom_pairs[0][:, None] == atom_ids[None, :]).astype(jnp.float32)
    tail_hit = (atom_pairs[1][:, None] == atom_ids[None, :]).astype(jnp.float32)
    return head_hit - tail_hit

def lattice_coords(atom_count):
    atom_ids = jnp.arange(atom_count, dtype=jnp.int32)
    lattice = jnp.stack([atom_ids % 4, atom_ids // 4 % 4, atom_ids // 16]).astype(jnp.float32)
    return (1.5 * lattice).reshape(1, 3 * atom_count)

def describe(coords, incidence):
    atom_count = incidence.shape[1]
    spatial = coords.reshape(coords.shape[0], 3, atom_count)
    offsets = jnp.einsum('bca,pa->bcp', spatial, incidence, precision=lax.Precision.HIGHEST)
    length = jnp.sqrt(lax.optimization_barrier(jnp.sum(offsets * offsets, axis=1)))
    return (1.0 / length, offsets / (length ** 3)[:, None, :])

def centered(coords, incidence):
    values, gradients = describe(coords, incidence)
    lattice_values = describe(lattice_coords(incidence.shape[1]), incidence)[0]
    return ((values - lattice_values).astype(jnp.bfloat16), gradients)

def to_desc(gradients, vectors, incidence):
    atom_count = incidence.shape[1]
    shifted = jnp.einsum('bca,pa->bcp', vectors.reshape(vectors.shape[0], 3, atom_count), incidence, precision=lax.Precision.HIGHEST)
    return -lax.optimization_barrier(jnp.sum(gradients * shifted, axis=1))

def to_forces(gradients, values, incidence):
    weighted = gradients * values[:, None, :]
    summed = jnp.einsum('bcp,pa->bca', weighted, incidence, precision=lax.Precision.HIGHEST)
    return -summed.reshape(values.shape[0], -1)

def matern(row_desc, col_desc, length):
    inner_prod = jnp.dot(row_desc, col_desc.T, preferred_element_type=jnp.float32)
    row_sq = lax.optimization_barrier(jnp.sum(jnp.square(row_desc.astype(jnp.float32)), axis=1))
    col_sq = lax.optimization_barrier(jnp.sum(jnp.square(col_desc.astype(jnp.float32)), axis=1))
    radius = jnp.sqrt(row_sq[:, None] + col_sq[None, :] - 2.0 * inner_prod) / length
    falloff = jnp.exp(-root_five * radius)
    diag_part = 5.0 / (3.0 * length ** 2) * (1.0 + root_five * radius) * falloff
    outer_part = 25.0 / (3.0 * length ** 4) * falloff
    return (diag_part, outer_part)

def apply_forward(train_desc, induce_desc, diag_part, outer_part, induce_vals):
    self_dot = lax.optimization_barrier(jnp.sum(induce_desc.astype(jnp.float32) * induce_vals.astype(jnp.float32), axis=1))
    projected = jnp.dot(train_desc, induce_vals.T, preferred_element_type=jnp.float32) - self_dot[None, :]
    product = outer_part * projected
    result = jnp.dot(diag_part.astype(jnp.bfloat16), induce_vals, preferred_element_type=jnp.float32)
    result = result + jnp.dot(product.astype(jnp.bfloat16), induce_desc, preferred_element_type=jnp.float32)
    return result - train_desc.astype(jnp.float32) * lax.optimization_barrier(jnp.sum(product, axis=1))[:, None]

def apply_adjoint(train_desc, induce_desc, diag_part, outer_part, train_vals):
    self_dot = lax.optimization_barrier(jnp.sum(train_desc.astype(jnp.float32) * train_vals.astype(jnp.float32), axis=1))
    projected = self_dot[:, None] - jnp.dot(train_vals, induce_desc.T, preferred_element_type=jnp.float32)
    product = outer_part * projected
    result = jnp.dot(diag_part.astype(jnp.bfloat16).T, train_vals, preferred_element_type=jnp.float32)
    result = result - jnp.dot(product.astype(jnp.bfloat16).T, train_desc, preferred_element_type=jnp.float32)
    return result + induce_desc.astype(jnp.float32) * lax.optimization_barrier(jnp.sum(product, axis=0))[:, None]

def reference(train_coords, induce_coords, train_forces, atom_pairs, length_scale):
    atom_count = train_coords.shape[1] // 3
    incidence = make_incidence(atom_pairs, atom_count)
    train_desc, train_grad = centered(train_coords, incidence)
    induce_desc, induce_grad = centered(induce_coords, incidence)
    length = length_scale[0]
    desc_rows = train_desc.reshape(N_TRAIN, TRAIN_DEV, DESC)
    grad_rows = train_grad.reshape(N_TRAIN, TRAIN_DEV, 3, DESC)

    def forward(vectors):
        induce_vals = to_desc(induce_grad, vectors, incidence).astype(jnp.bfloat16)

        def one_section(section):
            desc_sec, grad_sec = section
            diag_part, outer_part = matern(desc_sec, induce_desc, length)
            return to_forces(grad_sec, apply_forward(desc_sec, induce_desc, diag_part, outer_part, induce_vals), incidence)
        return lax.map(one_section, (desc_rows, grad_rows)).reshape(TRAIN_ALL, COMP)

    def adjoint(forces_like):
        train_vals = to_desc(train_grad, forces_like, incidence).astype(jnp.bfloat16).reshape(N_TRAIN, TRAIN_DEV, DESC)

        def add_section(running, section):
            desc_sec, vals_sec = section
            diag_part, outer_part = matern(desc_sec, induce_desc, length)
            return (running + apply_adjoint(desc_sec, induce_desc, diag_part, outer_part, vals_sec), None)
        running, unused = lax.scan(add_section, jnp.zeros((INDUCE_ALL, DESC), jnp.float32), (desc_rows, train_vals))
        return to_forces(induce_grad, running, incidence)
    start = adjoint(train_forces)
    probed = forward(start)
    quotient = jnp.sum(probed * probed) / jnp.sum(train_forces * probed)
    center = 0.775 * quotient
    spread = 0.725 * quotient
    momentum = spread / center
    direction = start / center
    coefficients = direction
    residual = start - adjoint(probed) / center
    for repeat in range(STEPS - 1):
        momentum_next = 1.0 / (2.0 * center / spread - momentum)
        direction = momentum_next * momentum * direction + 2.0 * momentum_next / spread * residual
        coefficients = coefficients + direction
        residual = residual - adjoint(forward(direction))
        momentum = momentum_next
    desc_coeffs = to_desc(induce_grad, coefficients, incidence)
    return (coefficients, residual, desc_coeffs)
```

```python
import functools
import math

import jax
import jax.numpy as jnp
from jax import lax
from jax.experimental import pallas as pl
from jax.experimental.pallas import tpu as pltpu
from jax.sharding import PartitionSpec as P

root_five = math.sqrt(5.0)
f32 = jnp.float32
bf16 = jnp.bfloat16
BLOCK = 128
CHUNK = 512
GATHER = 4
VMEM_LIMIT = 60 * 1024 * 1024


def dot(lhs, rhs, rhs_contract=0):
    return lax.dot_general(
        lhs, rhs, (((1,), (rhs_contract,)), ((), ())), preferred_element_type=f32
    )


def split_three(x):
    high = x.astype(bf16)
    rest = x - high.astype(f32)
    mid = rest.astype(bf16)
    low = (rest - mid.astype(f32)).astype(bf16)
    return jnp.concatenate([high, mid, low], axis=1)


def put_split(split_ref, start, values, atoms):
    rows = values.shape[0]
    for comp in range(3):
        part = values[:, comp * atoms : (comp + 1) * atoms]
        split_ref[comp, pl.ds(start, rows), :] = split_three(part)


def build_incidence(pairs_ref, inc_ref, inc_t_ref):
    atoms = inc_t_ref.shape[1]
    count = pairs_ref.shape[1]
    wide = inc_ref.shape[1]
    ids = lax.broadcasted_iota(jnp.int32, (atoms, count), 0)
    signs = (pairs_ref[0:1, :] == ids).astype(f32) - (pairs_ref[1:2, :] == ids).astype(f32)
    if wide > count:
        signs = jnp.concatenate([signs, jnp.zeros((atoms, wide - count), f32)], axis=1)
    for copy in range(3):
        inc_ref[copy * atoms : (copy + 1) * atoms, :] = signs.astype(bf16)
    inc_t_ref[...] = signs.T.astype(bf16)


def lattice_inverse(inc_ref, atoms, count):
    wide = inc_ref.shape[1]
    ids = lax.broadcasted_iota(jnp.int32, (8, atoms), 1)
    total = jnp.zeros((8, wide), f32)
    for steps in (ids % 4, ids // 4 % 4, ids // 16):
        part = dot((1.5 * steps.astype(f32)).astype(bf16), inc_ref[0:atoms, :])
        total = total + part * part
    lanes = lax.broadcasted_iota(jnp.int32, (8, wide), 1)
    padding = (lanes >= count).astype(f32)
    return lax.rsqrt(total + padding)[0:1, :], padding[0:1, :]


def loop(rows, body):
    block = min(rows, BLOCK)
    if rows == block:
        body(0, block)
        return

    def step(index, carry):
        body(pl.multiple_of(index * block, block), block)
        return carry

    lax.fori_loop(0, rows // block, step, 0)


def describe(split_ref, inc_ref, lat_ref, grad_ref, desc_ref, sq_ref):
    rows, wide = desc_ref.shape

    def body(start, block):
        lhs = split_ref[:, pl.ds(start, block), :].reshape(3 * block, -1)
        sq = jnp.zeros((block, 128), f32)
        for at in range(0, wide, CHUNK):
            cols = slice(at, at + CHUNK)
            off = dot(lhs, inc_ref[:, cols])
            off = [off[c * block : (c + 1) * block] for c in range(3)]
            inv = lax.rsqrt(
                off[0] * off[0] + off[1] * off[1] + off[2] * off[2] + lat_ref[1:2, cols]
            )
            desc = (inv - lat_ref[0:1, cols]).astype(bf16)
            desc_ref[pl.ds(start, block), cols] = desc
            cube = -(inv * inv * inv)
            for comp in range(3):
                grad_ref[comp, pl.ds(start, block), cols] = (off[comp] * cube).astype(grad_ref.dtype)
            wide_desc = desc.astype(f32)
            wide_desc = wide_desc * wide_desc
            for lane in range(0, CHUNK, 128):
                sq = sq + wide_desc[:, lane : lane + 128]
        sq_ref[pl.ds(start, block), :] = jnp.broadcast_to(
            jnp.sum(sq, axis=1, keepdims=True), (block, 128)
        )

    loop(rows, body)


def to_desc(split_ref, inc_ref, grad_ref, desc_ref, out_ref, self_ref):
    rows, wide = out_ref.shape

    def body(start, block):
        lhs = split_ref[:, pl.ds(start, block), :].reshape(3 * block, -1)
        total = jnp.zeros((block, 128), f32)
        for at in range(0, wide, CHUNK):
            cols = slice(at, at + CHUNK)
            diff = dot(lhs, inc_ref[:, cols])
            value = jnp.zeros((block, CHUNK), f32)
            for comp in range(3):
                grad = grad_ref[comp, pl.ds(start, block), cols].astype(f32)
                value = value + grad * diff[comp * block : (comp + 1) * block]
            value = value.astype(bf16)
            out_ref[pl.ds(start, block), cols] = value
            product = value.astype(f32) * desc_ref[pl.ds(start, block), cols].astype(f32)
            for lane in range(0, CHUNK, 128):
                total = total + product[:, lane : lane + 128]
        self_ref[pl.ds(start, block), :] = jnp.broadcast_to(
            jnp.sum(total, axis=1, keepdims=True), (block, 128)
        )

    loop(rows, body)


def mix_to_forces(diag_ref, vals_ref, cross_ref, desc_ref, own_ref, sum_ref, grad_ref, inc_t_ref, put):
    rows = own_ref.shape[0]
    wide = own_ref.shape[1]

    def body(start, block):
        diag = diag_ref[pl.ds(start, block), :]
        cross = cross_ref[pl.ds(start, block), :]
        sums = sum_ref[pl.ds(start, block), 0:1]
        forces = None
        for at in range(0, wide, CHUNK):
            cols = slice(at, at + CHUNK)
            value = dot(diag, vals_ref[:, cols]) + dot(cross, desc_ref[:, cols])
            value = value - own_ref[pl.ds(start, block), cols].astype(f32) * sums
            parts = []
            for comp in range(3):
                grad = grad_ref[comp, pl.ds(start, block), cols].astype(f32)
                parts.append((grad * value).astype(bf16))
            part = dot(jnp.concatenate(parts, axis=0), inc_t_ref[cols, :])
            forces = part if forces is None else forces + part
        put(start, block, [forces[c * block : (c + 1) * block] for c in range(3)])

    loop(rows, body)


def lane_sum(x):
    return jnp.broadcast_to(jnp.sum(x, axis=1, keepdims=True), (x.shape[0], 128))


def adjoint(ctx, put):
    to_desc(ctx.vec_t, ctx.inc, ctx.grad_t, ctx.desc_t, ctx.vals_t, ctx.self_t)
    rows = ctx.desc_t.shape[0]
    block = min(rows, 256)
    for at in range(0, rows, block):
        span = slice(at, at + block)
        project = dot(ctx.vals_t[span, :], ctx.desc_i[...], 1) - ctx.self_t[span, 0:1]
        product = (ctx.outer[span, :] * project).T
        ctx.cross_i[:, span] = product.astype(bf16)
        total = lane_sum(product)
        ctx.sum_i[...] = total if at == 0 else ctx.sum_i[...] + total
    mix_to_forces(
        ctx.diag_i, ctx.vals_t, ctx.cross_i, ctx.desc_t, ctx.desc_i, ctx.sum_i, ctx.grad_i, ctx.inc_t, put
    )


def forward(ctx, put):
    to_desc(ctx.vec_i, ctx.inc, ctx.grad_i, ctx.desc_i, ctx.vals_i, ctx.self_i)
    rows = ctx.desc_t.shape[0]
    block = min(rows, 256)
    self_row = ctx.self_i[...].T[0:1, :]
    for at in range(0, rows, block):
        span = slice(at, at + block)
        project = dot(ctx.desc_t[span, :], ctx.vals_i[...], 1) - self_row
        product = ctx.outer[span, :] * project
        ctx.cross_t[span, :] = product.astype(bf16)
        ctx.sum_t[span, :] = lane_sum(product)
    mix_to_forces(
        ctx.diag_t, ctx.vals_i, ctx.cross_t, ctx.desc_i, ctx.desc_t, ctx.sum_t, ctx.grad_t, ctx.inc_t, put
    )


def matern(ctx, length):
    rows = ctx.desc_t.shape[0]
    block = min(rows, 256)
    col_sq = ctx.self_i[...].T[0:1, :]
    for at in range(0, rows, block):
        span = slice(at, at + block)
        inner = dot(ctx.desc_t[span, :], ctx.desc_i[...], 1)
        square = ctx.self_t[span, 0:1] + col_sq - 2.0 * inner
        radius = root_five * (jnp.sqrt(jnp.maximum(square, 0.0)) / length)
        falloff = jnp.exp(-radius)
        diag = 5.0 / (3.0 * length**2) * (1.0 + radius) * falloff
        ctx.diag_t[span, :] = diag.astype(bf16)
        ctx.diag_i[:, span] = diag.T.astype(bf16)
        ctx.outer[span, :] = 25.0 / (3.0 * length**4) * falloff


class Ctx:
    def __init__(self, names, refs):
        for name, ref in zip(names, refs):
            setattr(self, name, ref)


def scratch_of(rows_t, rows_i, wide, atoms, names):
    kinds = dict(
        inc=((3 * atoms, wide), bf16),
        inc_t=((wide, atoms), bf16),
        lat=((8, wide), f32),
        vec_t=((3, rows_t, 3 * atoms), bf16),
        vec_i=((3, rows_i, 3 * atoms), bf16),
        vals_t=((rows_t, wide), bf16),
        vals_i=((rows_i, wide), bf16),
        self_t=((rows_t, 128), f32),
        self_i=((rows_i, 128), f32),
        sum_t=((rows_t, 128), f32),
        sum_i=((rows_i, 128), f32),
        cross_t=((rows_t, rows_i), bf16),
        cross_i=((rows_i, rows_t), bf16),
    )
    return [pltpu.VMEM(*kinds[name]) for name in names]


def first_kernel(n_train, n_induce, atoms, out_names, scratch_names, *refs):
    coords_t = refs[:n_train]
    forces_t = refs[n_train : 2 * n_train]
    coords_i = refs[2 * n_train : 2 * n_train + n_induce]
    pairs, length_ref = refs[2 * n_train + n_induce : 2 * n_train + n_induce + 2]
    rest = refs[2 * n_train + n_induce + 2 :]
    partial, start_out = rest[:2]
    ctx = Ctx(out_names + scratch_names, rest[2:])
    build_incidence(pairs, ctx.inc, ctx.inc_t)
    lattice, padding = lattice_inverse(ctx.inc, atoms, pairs.shape[1])
    ctx.lat[0:1, :] = lattice
    ctx.lat[1:2, :] = padding
    rows = coords_t[0].shape[0]
    for index, ref in enumerate(coords_t):
        put_split(ctx.vec_t, index * rows, ref[...], atoms)
    describe(ctx.vec_t, ctx.inc, ctx.lat, ctx.grad_t, ctx.desc_t, ctx.self_t)
    for index, ref in enumerate(forces_t):
        put_split(ctx.vec_t, index * rows, ref[...], atoms)
    rows = coords_i[0].shape[0]
    for index, ref in enumerate(coords_i):
        put_split(ctx.vec_i, index * rows, ref[...], atoms)
    describe(ctx.vec_i, ctx.inc, ctx.lat, ctx.grad_i, ctx.desc_i, ctx.self_i)
    matern(ctx, length_ref[0])

    def put_start(start, block, parts):
        for comp in range(3):
            start_out[pl.ds(start, block), comp * atoms : (comp + 1) * atoms] = parts[comp]
            ctx.vec_i[comp, pl.ds(start, block), :] = split_three(parts[comp])

    adjoint(ctx, put_start)

    def put_partial(start, block, parts):
        for comp in range(3):
            partial[pl.ds(start, block), comp * atoms : (comp + 1) * atoms] = parts[comp]

    forward(ctx, put_partial)


def second_kernel(n_sum, n_train, atoms, in_names, scratch_names, *refs):
    parts_in = refs[:n_sum]
    forces_t = refs[n_sum : n_sum + n_train]
    rest = refs[n_sum + n_train :]
    pairs, start_in = rest[:2]
    n_in = len(in_names)
    ctx = Ctx(in_names, rest[2 : 2 + n_in])
    partial, coeffs_out, resid_out = rest[2 + n_in : 5 + n_in]
    for name, ref in zip(scratch_names, rest[5 + n_in :]):
        setattr(ctx, name, ref)
    build_incidence(pairs, ctx.inc, ctx.inc_t)
    rows = forces_t[0].shape[0]
    probed_sq = jnp.zeros((1, 1), f32)
    cross_sq = jnp.zeros((1, 1), f32)
    for index in range(n_train):
        span = slice(index * rows, (index + 1) * rows)
        probed = parts_in[0][span, :]
        for ref in parts_in[1:]:
            probed = probed + ref[span, :]
        put_split(ctx.vec_t, index * rows, probed, atoms)
        probed_sq = probed_sq + jnp.sum(probed * probed, keepdims=True)
        cross_sq = cross_sq + jnp.sum(forces_t[index][...] * probed, keepdims=True)
    quotient = probed_sq / cross_sq
    center = 0.775 * quotient
    spread = 0.725 * quotient
    momentum = spread / center
    momentum_next = 1.0 / (2.0 * center / spread - momentum)

    def put_resid(start, block, parts):
        for comp in range(3):
            cols = slice(comp * atoms, (comp + 1) * atoms)
            first = start_in[pl.ds(start, block), cols]
            resid = first - parts[comp] / center
            direction = first / center
            coeffs = direction
            direction = momentum_next * momentum * direction + 2.0 * momentum_next / spread * resid
            resid_out[pl.ds(start, block), cols] = resid
            coeffs_out[pl.ds(start, block), cols] = coeffs + direction
            ctx.vec_i[comp, pl.ds(start, block), :] = split_three(direction)

    adjoint(ctx, put_resid)

    def put_partial(start, block, parts):
        for comp in range(3):
            partial[pl.ds(start, block), comp * atoms : (comp + 1) * atoms] = parts[comp]

    forward(ctx, put_partial)


def desc_kernel(atoms, coeffs, pairs, grad_i, coeffs_out, out, inc, inc_t, vec):
    build_incidence(pairs, inc, inc_t)
    put_split(vec, 0, coeffs[...], atoms)
    coeffs_out[...] = coeffs[...]
    count = out.shape[1]

    def body(start, block):
        lhs = vec[:, pl.ds(start, block), :].reshape(3 * block, -1)
        for at in range(0, inc.shape[1], CHUNK):
            end = min(at + CHUNK, count)
            diff = dot(lhs, inc[:, at : at + CHUNK])
            value = jnp.zeros((block, CHUNK), f32)
            for comp in range(3):
                grad = grad_i[comp, pl.ds(start, block), at : at + CHUNK].astype(f32)
                value = value + grad * diff[comp * block : (comp + 1) * block]
            out[pl.ds(start, block), at:end] = value[:, : end - at]

    loop(out.shape[0], body)


def third_kernel(n_sum, atoms, in_names, scratch_names, *refs):
    parts_in = refs[:n_sum]
    pairs, resid_in = refs[n_sum : n_sum + 2]
    n_in = len(in_names)
    rest = refs[n_sum + 2 :]
    ctx = Ctx(in_names, rest[:n_in])
    resid_out = rest[n_in]
    for name, ref in zip(scratch_names, rest[n_in + 1 :]):
        setattr(ctx, name, ref)
    build_incidence(pairs, ctx.inc, ctx.inc_t)
    total = parts_in[0][...]
    for ref in parts_in[1:]:
        total = total + ref[...]
    put_split(ctx.vec_t, 0, total, atoms)

    def put_resid(start, block, parts):
        for comp in range(3):
            cols = slice(comp * atoms, (comp + 1) * atoms)
            resid_out[pl.ds(start, block), cols] = resid_in[pl.ds(start, block), cols] - parts[comp]

    adjoint(ctx, put_resid)


def whole(shape):
    return pl.BlockSpec(shape, lambda *_: (0,) * len(shape))


def call(body, ins, specs, outs, scratch):
    return pl.pallas_call(
        body,
        grid=(1,),
        in_specs=specs,
        out_specs=[whole(o.shape) for o in outs],
        out_shape=outs,
        scratch_shapes=scratch,
        compiler_params=pltpu.CompilerParams(vmem_limit_bytes=VMEM_LIMIT),
    )(*ins)


def per_device(n_train, n_induce, train_coords, induce_coords, train_forces, atom_pairs, length_scale):
    atoms = train_coords.shape[1] // 3
    count = atom_pairs.shape[1]
    wide = -(-count // CHUNK) * CHUNK
    gather = math.gcd(GATHER, n_induce // 2)
    rows_t = n_train * train_coords.shape[0]
    own = induce_coords.shape[0]
    rows_i = gather * own

    coords_i = [induce_coords] + [
        lax.ppermute(induce_coords, "induce", [(i, i ^ (2 * step)) for i in range(n_induce)])
        for step in range(1, gather)
    ]
    both = jnp.concatenate([train_coords, train_forces], axis=1)
    both = lax.all_gather(both, "train", axis=0, tiled=True)
    coords_t = [both[:, : 3 * atoms]]
    forces_t = [both[:, 3 * atoms :]]

    grad_dtype = f32 if (rows_t + rows_i) * wide * 12 <= 20 * 1024 * 1024 else bf16
    sds = jax.ShapeDtypeStruct
    kept_names = ["grad_t", "grad_i", "desc_t", "desc_i", "diag_t", "diag_i", "outer"]
    kept = [
        sds((3, rows_t, wide), grad_dtype),
        sds((3, rows_i, wide), grad_dtype),
        sds((rows_t, wide), bf16),
        sds((rows_i, wide), bf16),
        sds((rows_t, rows_i), bf16),
        sds((rows_i, rows_t), bf16),
        sds((rows_t, rows_i), f32),
    ]
    vec_t = sds((rows_t, 3 * atoms), f32)
    vec_i = sds((rows_i, 3 * atoms), f32)
    names = ["inc", "inc_t", "lat", "vec_t", "vec_i", "vals_t", "vals_i", "self_t", "self_i"]
    names += ["sum_t", "sum_i", "cross_t", "cross_i"]
    smem = pl.BlockSpec(memory_space=pltpu.SMEM)
    ins = coords_t + forces_t + coords_i + [atom_pairs]
    partial, start, *state = call(
        functools.partial(first_kernel, len(coords_t), len(coords_i), atoms, kept_names, names),
        ins + [length_scale],
        [whole(x.shape) for x in ins] + [smem],
        [vec_t, vec_i] + kept,
        scratch_of(rows_t, rows_i, wide, atoms, names),
    )

    def reduce_parts(x):
        step = 2 * gather
        while step < n_induce:
            x = x + lax.ppermute(x, "induce", [(i, i ^ step) for i in range(n_induce)])
            step *= 2
        return [x, lax.ppermute(x, "induce", [(i, i ^ 1) for i in range(n_induce)])]

    names = [name for name in names if name != "lat"]
    parts = reduce_parts(partial)
    ins = parts + forces_t + [atom_pairs, start] + state
    partial, coeffs, resid = call(
        functools.partial(second_kernel, len(parts), len(forces_t), atoms, kept_names, names),
        ins,
        [whole(x.shape) for x in ins],
        [vec_t, vec_i, vec_i],
        scratch_of(rows_t, rows_i, wide, atoms, names),
    )
    own_vec = sds((own, 3 * atoms), f32)
    coeffs, desc_coeffs = call(
        functools.partial(desc_kernel, atoms),
        [coeffs, atom_pairs, state[1]],
        [whole(own_vec.shape), whole(atom_pairs.shape), whole((3, own, wide))],
        [own_vec, sds((own, count), f32)],
        scratch_of(rows_t, own, wide, atoms, ["inc", "inc_t", "vec_i"]),
    )
    names = ["inc", "inc_t", "vec_t", "vals_t", "self_t", "sum_i", "cross_i"]
    parts = reduce_parts(partial)
    in_names = ["grad_t", "grad_i", "desc_t", "desc_i", "diag_i", "outer"]
    ins = parts + [atom_pairs, resid] + state[:4] + state[5:]
    specs = [whole(x.shape) for x in parts + [atom_pairs]]
    specs += [whole(own_vec.shape), whole(kept[0].shape), whole((3, own, wide)), whole(kept[2].shape)]
    specs += [whole((own, wide)), whole((own, rows_t)), whole((rows_t, own))]
    (resid,) = call(
        functools.partial(third_kernel, len(parts), atoms, in_names, names),
        ins,
        specs,
        [own_vec],
        scratch_of(rows_t, own, wide, atoms, names),
    )
    return (coeffs, resid, desc_coeffs)


def solution(mesh):
    in_specs = (P("train", None), P("induce", None), P("train", None), P(), P())
    out_specs = (P("induce", None), P("induce", None), P("induce", None))
    body = functools.partial(per_device, mesh.shape["train"], mesh.shape["induce"])
    return jax.shard_map(
        body, mesh=mesh, in_specs=in_specs, out_specs=out_specs, check_vma=False
    )
```

```python
import functools
import math

import jax
import jax.numpy as jnp
from jax import lax
from jax.experimental import pallas as pl
from jax.experimental.pallas import tpu as pltpu
from jax.sharding import PartitionSpec as P

root_five = math.sqrt(5.0)
f32 = jnp.float32
bf16 = jnp.bfloat16
BLOCK = 128
CHUNK = 512
GATHER = 4
MIB = 1024 * 1024


def dot(lhs, rhs, rhs_contract=0):
    return lax.dot_general(
        lhs, rhs, (((1,), (rhs_contract,)), ((), ())), preferred_element_type=f32
    )


def split_three(x):
    high = x.astype(bf16)
    rest = x - high.astype(f32)
    mid = rest.astype(bf16)
    low = (rest - mid.astype(f32)).astype(bf16)
    return jnp.concatenate([high, mid, low], axis=1)


def put_split(split_ref, start, values, atoms):
    rows = values.shape[0]
    for comp in range(3):
        part = values[:, comp * atoms : (comp + 1) * atoms]
        split_ref[comp, pl.ds(start, rows), :] = split_three(part)


def build_incidence(pairs_ref, inc_ref, inc_t_ref):
    atoms = inc_t_ref.shape[1]
    count = pairs_ref.shape[1]
    wide = inc_ref.shape[1]
    ids = lax.broadcasted_iota(jnp.int32, (atoms, count), 0)
    signs = (pairs_ref[0:1, :] == ids).astype(f32) - (pairs_ref[1:2, :] == ids).astype(f32)
    if wide > count:
        signs = jnp.concatenate([signs, jnp.zeros((atoms, wide - count), f32)], axis=1)
    for copy in range(3):
        inc_ref[copy * atoms : (copy + 1) * atoms, :] = signs.astype(bf16)
    inc_t_ref[...] = signs.T.astype(bf16)


def lattice_inverse(inc_ref, atoms, count):
    wide = inc_ref.shape[1]
    ids = lax.broadcasted_iota(jnp.int32, (8, atoms), 1)
    total = jnp.zeros((8, wide), f32)
    for steps in (ids % 4, ids // 4 % 4, ids // 16):
        part = dot((1.5 * steps.astype(f32)).astype(bf16), inc_ref[0:atoms, :])
        total = total + part * part
    lanes = lax.broadcasted_iota(jnp.int32, (8, wide), 1)
    padding = (lanes >= count).astype(f32)
    return lax.rsqrt(total + padding)[0:1, :], padding[0:1, :]


def loop(rows, body):
    block = min(rows, BLOCK)
    if rows == block:
        body(0, block)
        return

    def step(index, carry):
        body(pl.multiple_of(index * block, block), block)
        return carry

    lax.fori_loop(0, rows // block, step, 0)


def describe(split_ref, inc_ref, lat_ref, grad_ref, desc_ref, sq_ref):
    rows, wide = desc_ref.shape

    def body(start, block):
        lhs = split_ref[:, pl.ds(start, block), :].reshape(3 * block, -1)
        sq = jnp.zeros((block, 128), f32)
        for at in range(0, wide, CHUNK):
            cols = slice(at, at + CHUNK)
            off = dot(lhs, inc_ref[:, cols])
            off = [off[c * block : (c + 1) * block] for c in range(3)]
            inv = lax.rsqrt(
                off[0] * off[0] + off[1] * off[1] + off[2] * off[2] + lat_ref[1:2, cols]
            )
            desc = (inv - lat_ref[0:1, cols]).astype(bf16)
            desc_ref[pl.ds(start, block), cols] = desc
            cube = -(inv * inv * inv)
            for comp in range(3):
                grad_ref[comp, pl.ds(start, block), cols] = (off[comp] * cube).astype(grad_ref.dtype)
            wide_desc = desc.astype(f32)
            wide_desc = wide_desc * wide_desc
            for lane in range(0, CHUNK, 128):
                sq = sq + wide_desc[:, lane : lane + 128]
        sq_ref[pl.ds(start, block), :] = jnp.broadcast_to(
            jnp.sum(sq, axis=1, keepdims=True), (block, 128)
        )

    loop(rows, body)


def to_desc(split_ref, inc_ref, grad_ref, desc_ref, out_ref, self_ref):
    rows, wide = out_ref.shape

    def body(start, block):
        lhs = split_ref[:, pl.ds(start, block), :].reshape(3 * block, -1)
        total = jnp.zeros((block, 128), f32)
        for at in range(0, wide, CHUNK):
            cols = slice(at, at + CHUNK)
            diff = dot(lhs, inc_ref[:, cols])
            value = jnp.zeros((block, CHUNK), f32)
            for comp in range(3):
                grad = grad_ref[comp, pl.ds(start, block), cols].astype(f32)
                value = value + grad * diff[comp * block : (comp + 1) * block]
            value = value.astype(bf16)
            out_ref[pl.ds(start, block), cols] = value
            product = value.astype(f32) * desc_ref[pl.ds(start, block), cols].astype(f32)
            for lane in range(0, CHUNK, 128):
                total = total + product[:, lane : lane + 128]
        self_ref[pl.ds(start, block), :] = jnp.broadcast_to(
            jnp.sum(total, axis=1, keepdims=True), (block, 128)
        )

    loop(rows, body)


def mix_to_forces(diag_ref, vals_ref, cross_ref, desc_ref, own_ref, sum_ref, grad_ref, inc_t_ref, put):
    rows = own_ref.shape[0]
    wide = own_ref.shape[1]

    def body(start, block):
        diag = diag_ref[pl.ds(start, block), :]
        cross = cross_ref[pl.ds(start, block), :]
        sums = sum_ref[pl.ds(start, block), 0:1]
        forces = None
        for at in range(0, wide, CHUNK):
            cols = slice(at, at + CHUNK)
            value = dot(diag, vals_ref[:, cols]) + dot(cross, desc_ref[:, cols])
            value = value - own_ref[pl.ds(start, block), cols].astype(f32) * sums
            parts = []
            for comp in range(3):
                grad = grad_ref[comp, pl.ds(start, block), cols].astype(f32)
                parts.append((grad * value).astype(bf16))
            part = dot(jnp.concatenate(parts, axis=0), inc_t_ref[cols, :])
            forces = part if forces is None else forces + part
        put(start, block, [forces[c * block : (c + 1) * block] for c in range(3)])

    loop(rows, body)


def lane_sum(x):
    return jnp.broadcast_to(jnp.sum(x, axis=1, keepdims=True), (x.shape[0], 128))


def adjoint(ctx, put):
    to_desc(ctx.vec_t, ctx.inc, ctx.grad_t, ctx.desc_t, ctx.vals_t, ctx.self_t)
    rows = ctx.desc_t.shape[0]
    block = min(rows, 256)
    for at in range(0, rows, block):
        span = slice(at, at + block)
        project = dot(ctx.vals_t[span, :], ctx.desc_i[...], 1) - ctx.self_t[span, 0:1]
        product = (ctx.outer[span, :] * project).T
        ctx.cross_i[:, span] = product.astype(bf16)
        total = lane_sum(product)
        ctx.sum_i[...] = total if at == 0 else ctx.sum_i[...] + total
    mix_to_forces(
        ctx.diag_i, ctx.vals_t, ctx.cross_i, ctx.desc_t, ctx.desc_i, ctx.sum_i, ctx.grad_i, ctx.inc_t, put
    )


def forward(ctx, put):
    to_desc(ctx.vec_i, ctx.inc, ctx.grad_i, ctx.desc_i, ctx.vals_i, ctx.self_i)
    rows = ctx.desc_t.shape[0]
    block = min(rows, 256)
    self_row = ctx.self_i[...].T[0:1, :]
    for at in range(0, rows, block):
        span = slice(at, at + block)
        project = dot(ctx.desc_t[span, :], ctx.vals_i[...], 1) - self_row
        product = ctx.outer[span, :] * project
        ctx.cross_t[span, :] = product.astype(bf16)
        ctx.sum_t[span, :] = lane_sum(product)
    mix_to_forces(
        ctx.diag_t, ctx.vals_i, ctx.cross_t, ctx.desc_i, ctx.desc_t, ctx.sum_t, ctx.grad_t, ctx.inc_t, put
    )


def matern(ctx, length):
    rows = ctx.desc_t.shape[0]
    block = min(rows, 256)
    col_sq = ctx.self_i[...].T[0:1, :]
    for at in range(0, rows, block):
        span = slice(at, at + block)
        inner = dot(ctx.desc_t[span, :], ctx.desc_i[...], 1)
        square = ctx.self_t[span, 0:1] + col_sq - 2.0 * inner
        radius = root_five * (jnp.sqrt(jnp.maximum(square, 0.0)) / length)
        falloff = jnp.exp(-radius)
        diag = 5.0 / (3.0 * length**2) * (1.0 + radius) * falloff
        ctx.diag_t[span, :] = diag.astype(bf16)
        ctx.diag_i[:, span] = diag.T.astype(bf16)
        ctx.outer[span, :] = 25.0 / (3.0 * length**4) * falloff


class Ctx:
    def __init__(self, names, refs):
        for name, ref in zip(names, refs):
            setattr(self, name, ref)


def scratch_of(rows_t, rows_i, wide, atoms, names):
    kinds = dict(
        inc=((3 * atoms, wide), bf16),
        inc_t=((wide, atoms), bf16),
        lat=((8, wide), f32),
        vec_t=((3, rows_t, 3 * atoms), bf16),
        vec_i=((3, rows_i, 3 * atoms), bf16),
        vals_t=((rows_t, wide), bf16),
        vals_i=((rows_i, wide), bf16),
        self_t=((rows_t, 128), f32),
        self_i=((rows_i, 128), f32),
        sum_t=((rows_t, 128), f32),
        sum_i=((rows_i, 128), f32),
        cross_t=((rows_t, rows_i), bf16),
        cross_i=((rows_i, rows_t), bf16),
    )
    return [pltpu.VMEM(*kinds[name]) for name in names]


def first_kernel(n_train, n_induce, atoms, out_names, scratch_names, *refs):
    coords_t = refs[:n_train]
    forces_t = refs[n_train : 2 * n_train]
    coords_i = refs[2 * n_train : 2 * n_train + n_induce]
    pairs, length_ref = refs[2 * n_train + n_induce : 2 * n_train + n_induce + 2]
    rest = refs[2 * n_train + n_induce + 2 :]
    partial, start_out = rest[:2]
    ctx = Ctx(out_names + scratch_names, rest[2:])
    build_incidence(pairs, ctx.inc, ctx.inc_t)
    lattice, padding = lattice_inverse(ctx.inc, atoms, pairs.shape[1])
    ctx.lat[0:1, :] = lattice
    ctx.lat[1:2, :] = padding
    rows = coords_t[0].shape[0]
    for index, ref in enumerate(coords_t):
        put_split(ctx.vec_t, index * rows, ref[...], atoms)
    describe(ctx.vec_t, ctx.inc, ctx.lat, ctx.grad_t, ctx.desc_t, ctx.self_t)
    for index, ref in enumerate(forces_t):
        put_split(ctx.vec_t, index * rows, ref[...], atoms)
    rows = coords_i[0].shape[1]
    for index, ref in enumerate(coords_i):
        put_split(ctx.vec_i, index * rows, ref[...].T, atoms)
    describe(ctx.vec_i, ctx.inc, ctx.lat, ctx.grad_i, ctx.desc_i, ctx.self_i)
    matern(ctx, length_ref[0])

    def put_start(start, block, parts):
        for comp in range(3):
            start_out[pl.ds(start, block), comp * atoms : (comp + 1) * atoms] = parts[comp]
            ctx.vec_i[comp, pl.ds(start, block), :] = split_three(parts[comp])

    adjoint(ctx, put_start)

    def put_partial(start, block, parts):
        for comp in range(3):
            partial[pl.ds(start, block), comp * atoms : (comp + 1) * atoms] = parts[comp]

    forward(ctx, put_partial)


def second_kernel(n_sum, n_train, atoms, in_names, scratch_names, *refs):
    parts_in = refs[:n_sum]
    forces_t = refs[n_sum : n_sum + n_train]
    rest = refs[n_sum + n_train :]
    pairs, start_in = rest[:2]
    n_in = len(in_names)
    ctx = Ctx(in_names, rest[2 : 2 + n_in])
    partial, coeffs_out, resid_out = rest[2 + n_in : 5 + n_in]
    for name, ref in zip(scratch_names, rest[5 + n_in :]):
        setattr(ctx, name, ref)
    build_incidence(pairs, ctx.inc, ctx.inc_t)
    rows = forces_t[0].shape[0]
    probed_sq = jnp.zeros((1, 1), f32)
    cross_sq = jnp.zeros((1, 1), f32)
    for index in range(n_train):
        span = slice(index * rows, (index + 1) * rows)
        probed = parts_in[0][span, :]
        for ref in parts_in[1:]:
            probed = probed + ref[span, :]
        put_split(ctx.vec_t, index * rows, probed, atoms)
        probed_sq = probed_sq + jnp.sum(probed * probed, keepdims=True)
        cross_sq = cross_sq + jnp.sum(forces_t[index][...] * probed, keepdims=True)
    quotient = probed_sq / cross_sq
    center = 0.775 * quotient
    spread = 0.725 * quotient
    momentum = spread / center
    momentum_next = 1.0 / (2.0 * center / spread - momentum)

    def put_resid(start, block, parts):
        for comp in range(3):
            cols = slice(comp * atoms, (comp + 1) * atoms)
            first = start_in[pl.ds(start, block), cols]
            resid = first - parts[comp] / center
            direction = first / center
            coeffs = direction
            direction = momentum_next * momentum * direction + 2.0 * momentum_next / spread * resid
            resid_out[pl.ds(start, block), cols] = resid
            coeffs_out[pl.ds(start, block), cols] = coeffs + direction
            ctx.vec_i[comp, pl.ds(start, block), :] = split_three(direction)

    adjoint(ctx, put_resid)

    def put_partial(start, block, parts):
        for comp in range(3):
            partial[pl.ds(start, block), comp * atoms : (comp + 1) * atoms] = parts[comp]

    forward(ctx, put_partial)


def desc_kernel(atoms, coeffs, pairs, grad_i, coeffs_out, out, inc, inc_t, vec):
    build_incidence(pairs, inc, inc_t)
    count, rows = out.shape
    own = coeffs[0:rows, :]
    put_split(vec, 0, own, atoms)
    coeffs_out[...] = own.T
    lhs = vec[...].reshape(3 * rows, -1)
    for at in range(0, inc.shape[1], CHUNK):
        end = min(at + CHUNK, count)
        diff = dot(lhs, inc[:, at : at + CHUNK])
        value = jnp.zeros((rows, CHUNK), f32)
        for comp in range(3):
            grad = grad_i[comp, 0:rows, at : at + CHUNK].astype(f32)
            value = value + grad * diff[comp * rows : (comp + 1) * rows]
        out[at:end, :] = value.T[: end - at, :]


def third_kernel(n_sum, atoms, in_names, scratch_names, *refs):
    parts_in = refs[:n_sum]
    pairs, resid_in = refs[n_sum : n_sum + 2]
    n_in = len(in_names)
    rest = refs[n_sum + 2 :]
    ctx = Ctx(in_names, rest[:n_in])
    resid_out = rest[n_in]
    for name, ref in zip(scratch_names, rest[n_in + 1 :]):
        setattr(ctx, name, ref)
    own = resid_out.shape[1]
    ctx.grad_i = ctx.grad_i.at[:, 0:own, :]
    ctx.desc_i = ctx.desc_i.at[0:own, :]
    ctx.diag_i = ctx.diag_i.at[0:own, :]
    ctx.outer = ctx.outer.at[:, 0:own]
    build_incidence(pairs, ctx.inc, ctx.inc_t)
    total = parts_in[0][...]
    for ref in parts_in[1:]:
        total = total + ref[...]
    put_split(ctx.vec_t, 0, total, atoms)

    def put_resid(start, block, parts):
        for comp in range(3):
            span = slice(comp * atoms, (comp + 1) * atoms)
            resid = resid_in[pl.ds(start, block), span] - parts[comp]
            resid_out[span, pl.ds(start, block)] = resid.T

    adjoint(ctx, put_resid)


def call(body, limit, ins, outs, scratch):
    vmem = pl.BlockSpec(memory_space=pltpu.VMEM)
    smem = pl.BlockSpec(memory_space=pltpu.SMEM)
    return pl.pallas_call(
        body,
        in_specs=[smem if x.ndim == 1 else vmem for x in ins],
        out_specs=[vmem for _ in outs],
        out_shape=outs,
        scratch_shapes=scratch,
        compiler_params=pltpu.CompilerParams(vmem_limit_bytes=limit),
    )(*ins)


def gather_rows(x, axis, size):
    others = [
        lax.ppermute(x, axis, [(i, i ^ step) for i in range(size)]) for step in range(1, size)
    ]
    return [x] + others


def per_device(n_train, n_induce, train_coords, induce_coords, train_forces, atom_pairs, length_scale):
    atoms = train_coords.shape[1] // 3
    count = atom_pairs.shape[1]
    wide = -(-count // CHUNK) * CHUNK
    gather = math.gcd(GATHER, n_induce // 2)
    rows_t = n_train * train_coords.shape[0]
    own = induce_coords.shape[0]
    rows_i = gather * own

    coords_t = gather_rows(train_coords, "train", n_train)
    forces_t = gather_rows(train_forces, "train", n_train)
    turned = induce_coords.T
    coords_i = [turned] + [
        lax.ppermute(turned, "induce", [(i, i ^ (2 * step)) for i in range(n_induce)])
        for step in range(1, gather)
    ]

    grad_dtype = f32 if (rows_t + rows_i) * wide * 12 <= 20 * MIB else bf16
    sds = jax.ShapeDtypeStruct
    kept_names = ["grad_t", "grad_i", "desc_t", "desc_i", "diag_t", "diag_i", "outer"]
    kept = [
        ((3, rows_t, wide), grad_dtype),
        ((3, rows_i, wide), grad_dtype),
        ((rows_t, wide), bf16),
        ((rows_i, wide), bf16),
        ((rows_t, rows_i), bf16),
        ((rows_i, rows_t), bf16),
        ((rows_t, rows_i), f32),
    ]
    size = sum(math.prod(shape) * jnp.dtype(dtype).itemsize for shape, dtype in kept)
    stays = size <= 30 * MIB and rows_t <= 256
    limit = 24 * MIB if stays else 60 * MIB
    kept = [(pltpu.VMEM if stays else sds)(shape, dtype) for shape, dtype in kept]
    vec_t = sds((rows_t, 3 * atoms), f32)
    vec_i = sds((rows_i, 3 * atoms), f32)
    names = ["inc", "inc_t", "lat", "vec_t", "vec_i", "vals_t", "vals_i", "self_t", "self_i"]
    names += ["sum_t", "sum_i", "cross_t", "cross_i"]
    partial, start, *state = call(
        functools.partial(first_kernel, len(coords_t), len(coords_i), atoms, kept_names, names),
        limit,
        coords_t + forces_t + coords_i + [atom_pairs, length_scale],
        [vec_t, vec_i] + kept,
        scratch_of(rows_t, rows_i, wide, atoms, names),
    )

    def reduce_parts(x):
        step = 2 * gather
        while step < n_induce:
            x = x + lax.ppermute(x, "induce", [(i, i ^ step) for i in range(n_induce)])
            step *= 2
        return [x, lax.ppermute(x, "induce", [(i, i ^ 1) for i in range(n_induce)])]

    names = [name for name in names if name != "lat"]
    parts = reduce_parts(partial)
    partial, coeffs, resid = call(
        functools.partial(second_kernel, len(parts), len(forces_t), atoms, kept_names, names),
        limit,
        parts + forces_t + [atom_pairs, start] + state,
        [vec_t, vec_i, vec_i],
        scratch_of(rows_t, rows_i, wide, atoms, names),
    )
    parts = reduce_parts(partial)
    own_vec = sds((3 * atoms, own), f32)
    coeffs, desc_coeffs = call(
        functools.partial(desc_kernel, atoms),
        limit,
        [coeffs, atom_pairs, state[1]],
        [own_vec, sds((count, own), f32)],
        scratch_of(rows_t, own, wide, atoms, ["inc", "inc_t", "vec_i"]),
    )
    names = ["inc", "inc_t", "vec_t", "vals_t", "self_t", "sum_i", "cross_i"]
    in_names = ["grad_t", "grad_i", "desc_t", "desc_i", "diag_i", "outer"]
    (resid,) = call(
        functools.partial(third_kernel, len(parts), atoms, in_names, names),
        limit,
        parts + [atom_pairs, resid] + state[:4] + state[5:],
        [own_vec],
        scratch_of(rows_t, own, wide, atoms, names),
    )
    return (coeffs.T, resid.T, desc_coeffs.T)


def solution(mesh):
    in_specs = (P("train", None), P("induce", None), P("train", None), P(), P())
    out_specs = (P("induce", None), P("induce", None), P("induce", None))
    body = functools.partial(per_device, mesh.shape["train"], mesh.shape["induce"])
    return jax.shard_map(
        body, mesh=mesh, in_specs=in_specs, out_specs=out_specs, check_vma=False
    )
```

```python
import functools
import math

import jax
import jax.numpy as jnp
from jax import lax
from jax.experimental import pallas as pl
from jax.experimental.pallas import tpu as pltpu
from jax.sharding import PartitionSpec as P

root_five = math.sqrt(5.0)
f32 = jnp.float32
bf16 = jnp.bfloat16
CHUNK = 256
DESCRIBE_BLOCK = 256
DESC_BLOCK = 256
MIX_BLOCK = 512
GATHER = 4
MIB = 1024 * 1024


def dot(lhs, rhs, rhs_contract=0):
    return lax.dot_general(
        lhs, rhs, (((1,), (rhs_contract,)), ((), ())), preferred_element_type=f32
    )


def split_three(x):
    high = x.astype(bf16)
    rest = x - high.astype(f32)
    mid = rest.astype(bf16)
    low = (rest - mid.astype(f32)).astype(bf16)
    return jnp.concatenate([high, mid, low], axis=1)


def put_split(split_ref, start, values, atoms):
    rows = values.shape[0]
    for comp in range(3):
        part = values[:, comp * atoms : (comp + 1) * atoms]
        split_ref[comp, pl.ds(start, rows), :] = split_three(part)


def build_incidence(pairs_ref, inc_ref, inc_t_ref):
    atoms = inc_t_ref.shape[1]
    count = pairs_ref.shape[1]
    wide = inc_ref.shape[1]
    ids = lax.broadcasted_iota(jnp.int32, (atoms, count), 0)
    signs = (pairs_ref[0:1, :] == ids).astype(f32) - (pairs_ref[1:2, :] == ids).astype(f32)
    if wide > count:
        signs = jnp.concatenate([signs, jnp.zeros((atoms, wide - count), f32)], axis=1)
    for copy in range(3):
        inc_ref[copy * atoms : (copy + 1) * atoms, :] = signs.astype(bf16)
    inc_t_ref[...] = signs.T.astype(bf16)


def lattice_inverse(inc_ref, atoms, count):
    wide = inc_ref.shape[1]
    ids = lax.broadcasted_iota(jnp.int32, (8, atoms), 1)
    total = jnp.zeros((8, wide), f32)
    for steps in (ids % 4, ids // 4 % 4, ids // 16):
        part = dot((1.5 * steps.astype(f32)).astype(bf16), inc_ref[0:atoms, :])
        total = total + part * part
    lanes = lax.broadcasted_iota(jnp.int32, (8, wide), 1)
    padding = (lanes >= count).astype(f32)
    return lax.rsqrt(total + padding)[0:1, :], padding[0:1, :]


def loop(rows, block, body):
    block = min(rows, block)
    if rows == block:
        body(0, block)
        return

    def step(index, carry):
        body(pl.multiple_of(index * block, block), block)
        return carry

    lax.fori_loop(0, rows // block, step, 0)


def describe(split_ref, inc_ref, lat_ref, grad_ref, desc_ref, sq_ref):
    rows, wide = desc_ref.shape

    def body(start, block):
        lhs = split_ref[:, pl.ds(start, block), :].reshape(3 * block, -1)
        sq = jnp.zeros((block, 128), f32)
        for at in range(0, wide, CHUNK):
            cols = slice(at, at + CHUNK)
            off = dot(lhs, inc_ref[:, cols])
            off = [off[c * block : (c + 1) * block] for c in range(3)]
            inv = lax.rsqrt(
                off[0] * off[0] + off[1] * off[1] + off[2] * off[2] + lat_ref[1:2, cols]
            )
            desc = (inv - lat_ref[0:1, cols]).astype(bf16)
            desc_ref[pl.ds(start, block), cols] = desc
            cube = -(inv * inv * inv)
            for comp in range(3):
                grad_ref[comp, pl.ds(start, block), cols] = (off[comp] * cube).astype(grad_ref.dtype)
            wide_desc = desc.astype(f32)
            wide_desc = wide_desc * wide_desc
            for lane in range(0, CHUNK, 128):
                sq = sq + wide_desc[:, lane : lane + 128]
        sq_ref[pl.ds(start, block), :] = jnp.broadcast_to(
            jnp.sum(sq, axis=1, keepdims=True), (block, 128)
        )

    loop(rows, DESCRIBE_BLOCK, body)


def to_desc(split_ref, inc_ref, grad_ref, desc_ref, out_ref, self_ref):
    rows, wide = out_ref.shape

    def body(start, block):
        lhs = split_ref[:, pl.ds(start, block), :].reshape(3 * block, -1)
        total = jnp.zeros((block, 128), f32)
        for at in range(0, wide, CHUNK):
            cols = slice(at, at + CHUNK)
            diff = dot(lhs, inc_ref[:, cols])
            value = jnp.zeros((block, CHUNK), f32)
            for comp in range(3):
                grad = grad_ref[comp, pl.ds(start, block), cols].astype(f32)
                value = value + grad * diff[comp * block : (comp + 1) * block]
            value = value.astype(bf16)
            out_ref[pl.ds(start, block), cols] = value
            product = value.astype(f32) * desc_ref[pl.ds(start, block), cols].astype(f32)
            for lane in range(0, CHUNK, 128):
                total = total + product[:, lane : lane + 128]
        self_ref[pl.ds(start, block), :] = jnp.broadcast_to(
            jnp.sum(total, axis=1, keepdims=True), (block, 128)
        )

    loop(rows, DESC_BLOCK, body)


def mix_to_forces(diag_ref, vals_ref, cross_ref, desc_ref, own_ref, sum_ref, grad_ref, inc_t_ref, put):
    rows = own_ref.shape[0]
    wide = own_ref.shape[1]

    def body(start, block):
        diag = diag_ref[pl.ds(start, block), :]
        cross = cross_ref[pl.ds(start, block), :]
        sums = sum_ref[pl.ds(start, block), 0:1]
        forces = None
        for at in range(0, wide, CHUNK):
            cols = slice(at, at + CHUNK)
            value = dot(diag, vals_ref[:, cols]) + dot(cross, desc_ref[:, cols])
            value = value - own_ref[pl.ds(start, block), cols].astype(f32) * sums
            parts = []
            for comp in range(3):
                grad = grad_ref[comp, pl.ds(start, block), cols].astype(f32)
                parts.append((grad * value).astype(bf16))
            part = dot(jnp.concatenate(parts, axis=0), inc_t_ref[cols, :])
            forces = part if forces is None else forces + part
        put(start, block, [forces[c * block : (c + 1) * block] for c in range(3)])

    loop(rows, MIX_BLOCK, body)


def lane_sum(x):
    return jnp.broadcast_to(jnp.sum(x, axis=1, keepdims=True), (x.shape[0], 128))


def adjoint(ctx, put):
    rows = ctx.desc_t.shape[0]
    block = min(rows, 256)
    for at in range(0, rows, block):
        span = slice(at, at + block)
        project = dot(ctx.vals_t[span, :], ctx.desc_i[...], 1) - ctx.self_t[span, 0:1]
        product = (ctx.outer[span, :] * project).T
        ctx.cross_i[:, span] = product.astype(bf16)
        total = lane_sum(product)
        ctx.sum_i[...] = total if at == 0 else ctx.sum_i[...] + total
    mix_to_forces(
        ctx.diag_i, ctx.vals_t, ctx.cross_i, ctx.desc_t, ctx.desc_i, ctx.sum_i, ctx.grad_i, ctx.inc_t, put
    )


def forward(ctx, put):
    to_desc(ctx.vec_i, ctx.inc, ctx.grad_i, ctx.desc_i, ctx.vals_i, ctx.self_i)
    rows = ctx.desc_t.shape[0]
    block = min(rows, 256)
    self_row = ctx.self_i[...].T[0:1, :]
    for at in range(0, rows, block):
        span = slice(at, at + block)
        project = dot(ctx.desc_t[span, :], ctx.vals_i[...], 1) - self_row
        product = ctx.outer[span, :] * project
        ctx.cross_t[span, :] = product.astype(bf16)
        ctx.sum_t[span, :] = lane_sum(product)
    mix_to_forces(
        ctx.diag_t, ctx.vals_i, ctx.cross_t, ctx.desc_i, ctx.desc_t, ctx.sum_t, ctx.grad_t, ctx.inc_t, put
    )


def matern(ctx, length):
    rows = ctx.desc_t.shape[0]
    block = min(rows, 256)
    col_sq = ctx.self_i[...].T[0:1, :]
    for at in range(0, rows, block):
        span = slice(at, at + block)
        inner = dot(ctx.desc_t[span, :], ctx.desc_i[...], 1)
        square = ctx.sq_t[span, 0:1] + col_sq - 2.0 * inner
        radius = root_five * (jnp.sqrt(jnp.maximum(square, 0.0)) / length)
        falloff = jnp.exp(-radius)
        diag = 5.0 / (3.0 * length**2) * (1.0 + radius) * falloff
        ctx.diag_t[span, :] = diag.astype(bf16)
        ctx.diag_i[:, span] = diag.T.astype(bf16)
        ctx.outer[span, :] = 25.0 / (3.0 * length**4) * falloff


class Ctx:
    def __init__(self, names, refs):
        for name, ref in zip(names, refs):
            setattr(self, name, ref)


def scratch_of(rows_t, rows_i, wide, atoms, names):
    kinds = dict(
        inc=((3 * atoms, wide), bf16),
        inc_t=((wide, atoms), bf16),
        lat=((8, wide), f32),
        vec_t=((3, rows_t, 3 * atoms), bf16),
        vec_i=((3, rows_i, 3 * atoms), bf16),
        vals_t=((rows_t, wide), bf16),
        vals_i=((rows_i, wide), bf16),
        self_t=((rows_t, 128), f32),
        self_i=((rows_i, 128), f32),
        sum_t=((rows_t, 128), f32),
        sum_i=((rows_i, 128), f32),
        cross_t=((rows_t, rows_i), bf16),
        cross_i=((rows_i, rows_t), bf16),
    )
    return [pltpu.VMEM(*kinds[name]) for name in names]


def join_kernel(coords, forces, turned, pairs, both_out, turned_out, pairs_out, left, right, sems):
    width = coords.shape[1]
    copies = [
        pltpu.make_async_copy(source, target, sems.at[index])
        for index, (source, target) in enumerate(
            ((coords, left), (forces, right), (turned, turned_out), (pairs, pairs_out))
        )
    ]
    for copy in copies:
        copy.start()
    for copy in copies:
        copy.wait()
    both_out[:, :width] = left[...]
    both_out[:, width:] = right[...]


def train_kernel(n_train, atoms, out_names, *refs):
    both_t = refs[:n_train]
    pairs = refs[n_train]
    ctx = Ctx(out_names + ["vec_t"], refs[n_train + 1 :])
    build_incidence(pairs, ctx.inc, ctx.inc_t)
    lattice, padding = lattice_inverse(ctx.inc, atoms, pairs.shape[1])
    ctx.lat[0:1, :] = lattice
    ctx.lat[1:2, :] = padding
    rows = both_t[0].shape[0]
    for index, ref in enumerate(both_t):
        put_split(ctx.vec_t, index * rows, ref[:, : 3 * atoms], atoms)
    describe(ctx.vec_t, ctx.inc, ctx.lat, ctx.grad_t, ctx.desc_t, ctx.sq_t)
    for index, ref in enumerate(both_t):
        put_split(ctx.vec_t, index * rows, ref[:, 3 * atoms :], atoms)
    to_desc(ctx.vec_t, ctx.inc, ctx.grad_t, ctx.desc_t, ctx.vals_t, ctx.self_t)


def first_kernel(n_induce, atoms, in_names, out_names, scratch_names, *refs):
    coords_i = refs[:n_induce]
    length_ref = refs[n_induce]
    n_in = n_induce + 1 + len(in_names)
    partial, start_out = refs[n_in : n_in + 2]
    ctx = Ctx(in_names + out_names + scratch_names, refs[n_induce + 1 : n_in] + refs[n_in + 2 :])
    rows = coords_i[0].shape[1]
    for index, ref in enumerate(coords_i):
        put_split(ctx.vec_i, index * rows, ref[...].T, atoms)
    describe(ctx.vec_i, ctx.inc, ctx.lat, ctx.grad_i, ctx.desc_i, ctx.self_i)
    matern(ctx, length_ref[0])

    def put_start(start, block, parts):
        for comp in range(3):
            start_out[pl.ds(start, block), comp * atoms : (comp + 1) * atoms] = parts[comp]
            ctx.vec_i[comp, pl.ds(start, block), :] = split_three(parts[comp])

    adjoint(ctx, put_start)

    def put_partial(start, block, parts):
        for comp in range(3):
            partial[pl.ds(start, block), comp * atoms : (comp + 1) * atoms] = parts[comp]

    forward(ctx, put_partial)


def second_kernel(n_sum, n_train, atoms, in_names, scratch_names, *refs):
    parts_in = refs[:n_sum]
    both_t = refs[n_sum : n_sum + n_train]
    rest = refs[n_sum + n_train :]
    start_in = rest[0]
    n_in = len(in_names)
    ctx = Ctx(in_names, rest[1 : 1 + n_in])
    partial, coeffs_out, resid_out = rest[1 + n_in : 4 + n_in]
    for name, ref in zip(scratch_names, rest[4 + n_in :]):
        setattr(ctx, name, ref)
    rows = both_t[0].shape[0]
    probed_sq = jnp.zeros((1, 1), f32)
    cross_sq = jnp.zeros((1, 1), f32)
    for index in range(n_train):
        span = slice(index * rows, (index + 1) * rows)
        probed = parts_in[0][span, :]
        for ref in parts_in[1:]:
            probed = probed + ref[span, :]
        put_split(ctx.vec_t, index * rows, probed, atoms)
        probed_sq = probed_sq + jnp.sum(probed * probed, keepdims=True)
        cross_sq = cross_sq + jnp.sum(both_t[index][:, 3 * atoms :] * probed, keepdims=True)
    quotient = probed_sq / cross_sq
    center = 0.775 * quotient
    spread = 0.725 * quotient
    momentum = spread / center
    momentum_next = 1.0 / (2.0 * center / spread - momentum)

    def put_resid(start, block, parts):
        for comp in range(3):
            cols = slice(comp * atoms, (comp + 1) * atoms)
            first = start_in[pl.ds(start, block), cols]
            resid = first - parts[comp] / center
            direction = first / center
            coeffs = direction
            direction = momentum_next * momentum * direction + 2.0 * momentum_next / spread * resid
            resid_out[pl.ds(start, block), cols] = resid
            coeffs_out[pl.ds(start, block), cols] = coeffs + direction
            ctx.vec_i[comp, pl.ds(start, block), :] = split_three(direction)

    to_desc(ctx.vec_t, ctx.inc, ctx.grad_t, ctx.desc_t, ctx.vals_t, ctx.self_t)
    adjoint(ctx, put_resid)

    def put_partial(start, block, parts):
        for comp in range(3):
            partial[pl.ds(start, block), comp * atoms : (comp + 1) * atoms] = parts[comp]

    forward(ctx, put_partial)


def desc_kernel(atoms, coeffs, inc, grad_i, coeffs_out, out, vec):
    count, rows = out.shape
    own = coeffs[0:rows, :]
    put_split(vec, 0, own, atoms)
    coeffs_out[...] = own.T
    lhs = vec[...].reshape(3 * rows, -1)
    for at in range(0, inc.shape[1], CHUNK):
        end = min(at + CHUNK, count)
        diff = dot(lhs, inc[:, at : at + CHUNK])
        value = jnp.zeros((rows, CHUNK), f32)
        for comp in range(3):
            grad = grad_i[comp, 0:rows, at : at + CHUNK].astype(f32)
            value = value + grad * diff[comp * rows : (comp + 1) * rows]
        out[at:end, :] = value.T[: end - at, :]


def third_kernel(n_sum, atoms, in_names, scratch_names, *refs):
    parts_in = refs[:n_sum]
    resid_in = refs[n_sum]
    n_in = len(in_names)
    rest = refs[n_sum + 1 :]
    ctx = Ctx(in_names, rest[:n_in])
    resid_out = rest[n_in]
    for name, ref in zip(scratch_names, rest[n_in + 1 :]):
        setattr(ctx, name, ref)
    own = resid_out.shape[1]
    ctx.grad_i = ctx.grad_i.at[:, 0:own, :]
    ctx.desc_i = ctx.desc_i.at[0:own, :]
    ctx.diag_i = ctx.diag_i.at[0:own, :]
    ctx.outer = ctx.outer.at[:, 0:own]
    total = parts_in[0][...]
    for ref in parts_in[1:]:
        total = total + ref[...]
    put_split(ctx.vec_t, 0, total, atoms)

    def put_resid(start, block, parts):
        for comp in range(3):
            span = slice(comp * atoms, (comp + 1) * atoms)
            resid = resid_in[pl.ds(start, block), span] - parts[comp]
            resid_out[span, pl.ds(start, block)] = resid.T

    to_desc(ctx.vec_t, ctx.inc, ctx.grad_t, ctx.desc_t, ctx.vals_t, ctx.self_t)
    adjoint(ctx, put_resid)


def call(body, limit, ins, outs, scratch, fetch=False):
    vmem = pl.BlockSpec(memory_space=pltpu.VMEM)
    smem = pl.BlockSpec(memory_space=pltpu.SMEM)
    hbm = pl.BlockSpec(memory_space=pl.ANY)
    return pl.pallas_call(
        body,
        in_specs=[hbm if fetch else smem if x.ndim == 1 else vmem for x in ins],
        out_specs=[vmem for _ in outs],
        out_shape=outs,
        scratch_shapes=scratch,
        compiler_params=pltpu.CompilerParams(vmem_limit_bytes=limit),
    )(*ins)


def gather_rows(x, axis, size):
    others = [
        lax.ppermute(x, axis, [(i, i ^ step) for i in range(size)]) for step in range(1, size)
    ]
    return [x] + others


def per_device(n_train, n_induce, train_coords, induce_coords, train_forces, atom_pairs, length_scale):
    atoms = train_coords.shape[1] // 3
    count = atom_pairs.shape[1]
    wide = -(-count // CHUNK) * CHUNK
    gather = math.gcd(GATHER, n_induce // 2)
    rows_t = n_train * train_coords.shape[0]
    own = induce_coords.shape[0]
    rows_i = gather * own
    grad_dtype = f32 if (rows_t + rows_i) * wide * 12 <= 20 * MIB else bf16
    kinds = dict(
        grad_t=((3, rows_t, wide), grad_dtype),
        grad_i=((3, rows_i, wide), grad_dtype),
        desc_t=((rows_t, wide), bf16),
        desc_i=((rows_i, wide), bf16),
        diag_t=((rows_t, rows_i), bf16),
        diag_i=((rows_i, rows_t), bf16),
        outer=((rows_t, rows_i), f32),
        inc=((3 * atoms, wide), bf16),
        inc_t=((wide, atoms), bf16),
        lat=((8, wide), f32),
        vals_t=((rows_t, wide), bf16),
        sq_t=((rows_t, 128), f32),
        self_t=((rows_t, 128), f32),
    )
    size = sum(math.prod(shape) * jnp.dtype(dtype).itemsize for shape, dtype in kinds.values())
    stays = size <= 32 * MIB and rows_t <= 256
    limit = 24 * MIB if stays else 60 * MIB
    sds = jax.ShapeDtypeStruct
    kept = pltpu.VMEM if stays else sds

    def pin(xs):
        return [pltpu.with_memory_space_constraint(x, pltpu.VMEM) for x in xs] if stays else xs

    both, turned, pairs = call(
        join_kernel,
        limit,
        [train_coords, train_forces, induce_coords.T, atom_pairs],
        [kept((train_coords.shape[0], 6 * atoms), f32), kept((3 * atoms, own), f32), kept(atom_pairs.shape, atom_pairs.dtype)],
        [pltpu.VMEM(train_coords.shape, f32)] * 2 + [pltpu.SemaphoreType.DMA((4,))],
        fetch=True,
    )
    both_t = gather_rows(both, "train", n_train)
    coords_i = [turned] + [
        lax.ppermute(turned, "induce", [(i, i ^ (2 * step)) for i in range(n_induce)])
        for step in range(1, gather)
    ]
    both_t = both_t[:1] + pin(both_t[1:])
    coords_i = coords_i[:1] + pin(coords_i[1:])

    train_names = ["grad_t", "desc_t", "inc", "inc_t", "lat", "vals_t", "sq_t", "self_t"]
    train_state = call(
        functools.partial(train_kernel, n_train, atoms, train_names),
        limit,
        both_t + [pairs],
        [kept(*kinds[name]) for name in train_names],
        scratch_of(rows_t, rows_i, wide, atoms, ["vec_t"]),
    )
    induce_names = ["grad_i", "desc_i", "diag_t", "diag_i", "outer"]
    names = ["vec_i", "vals_i", "self_i", "sum_t", "sum_i", "cross_t", "cross_i"]
    vec_t = sds((rows_t, 3 * atoms), f32)
    vec_i = sds((rows_i, 3 * atoms), f32)
    partial, start, *induce_state = call(
        functools.partial(first_kernel, gather, atoms, train_names, induce_names, names),
        limit,
        coords_i + [length_scale] + list(train_state),
        [vec_t, vec_i] + [kept(*kinds[name]) for name in induce_names],
        scratch_of(rows_t, rows_i, wide, atoms, names),
    )
    kept_names = ["grad_t", "desc_t", "inc", "inc_t"] + induce_names
    state = list(train_state[:4]) + list(induce_state)

    def reduce_parts(x):
        step = 2 * gather
        while step < n_induce:
            x = x + lax.ppermute(x, "induce", [(i, i ^ step) for i in range(n_induce)])
            step *= 2
        return pin([x, lax.ppermute(x, "induce", [(i, i ^ 1) for i in range(n_induce)])])

    names = ["vec_t", "vals_t", "self_t"] + names
    parts = reduce_parts(partial)
    partial, coeffs, resid = call(
        functools.partial(second_kernel, len(parts), n_train, atoms, kept_names, names),
        limit,
        parts + both_t + [start] + state,
        [vec_t, vec_i, vec_i],
        scratch_of(rows_t, rows_i, wide, atoms, names),
    )
    parts = reduce_parts(partial)
    own_vec = sds((3 * atoms, own), f32)
    coeffs, desc_coeffs = call(
        functools.partial(desc_kernel, atoms),
        limit,
        [coeffs, state[2], state[4]],
        [own_vec, sds((count, own), f32)],
        scratch_of(rows_t, own, wide, atoms, ["vec_i"]),
    )
    names = ["vec_t", "vals_t", "self_t", "sum_i", "cross_i"]
    in_names = kept_names
    (resid,) = call(
        functools.partial(third_kernel, len(parts), atoms, in_names, names),
        limit,
        parts + [resid] + state,
        [own_vec],
        scratch_of(rows_t, own, wide, atoms, names),
    )
    return (coeffs.T, resid.T, desc_coeffs.T)


def solution(mesh):
    in_specs = (P("train", None), P("induce", None), P("train", None), P(), P())
    out_specs = (P("induce", None), P("induce", None), P("induce", None))
    body = functools.partial(per_device, mesh.shape["train"], mesh.shape["induce"])
    return jax.shard_map(
        body, mesh=mesh, in_specs=in_specs, out_specs=out_specs, check_vma=False
    )
```

```python
import functools
import math

import jax
import jax.numpy as jnp
from jax import lax
from jax.experimental import pallas as pl
from jax.experimental.pallas import tpu as pltpu
from jax.sharding import PartitionSpec as P

root_five = math.sqrt(5.0)
f32 = jnp.float32
bf16 = jnp.bfloat16
CHUNK = 256
DESCRIBE_BLOCK = 256
DESC_BLOCK = 256
MIX_BLOCK = 512
GATHER = 4
MIB = 1024 * 1024


def dot(lhs, rhs, rhs_contract=0):
    return lax.dot_general(
        lhs, rhs, (((1,), (rhs_contract,)), ((), ())), preferred_element_type=f32
    )


def split_three(x):
    high = x.astype(bf16)
    rest = x - high.astype(f32)
    mid = rest.astype(bf16)
    low = (rest - mid.astype(f32)).astype(bf16)
    return jnp.concatenate([high, mid, low], axis=1)


def put_split(split_ref, start, values, atoms):
    rows = values.shape[0]
    for comp in range(3):
        part = values[:, comp * atoms : (comp + 1) * atoms]
        split_ref[comp, pl.ds(start, rows), :] = split_three(part)


def build_incidence(pairs_ref, inc_ref, inc_t_ref):
    atoms = inc_t_ref.shape[1]
    count = pairs_ref.shape[1]
    wide = inc_ref.shape[1]
    ids = lax.broadcasted_iota(jnp.int32, (atoms, count), 0)
    signs = (pairs_ref[0:1, :] == ids).astype(f32) - (pairs_ref[1:2, :] == ids).astype(f32)
    if wide > count:
        signs = jnp.concatenate([signs, jnp.zeros((atoms, wide - count), f32)], axis=1)
    for copy in range(3):
        inc_ref[copy * atoms : (copy + 1) * atoms, :] = signs.astype(bf16)
    inc_t_ref[...] = signs.T.astype(bf16)


def lattice_inverse(inc_ref, atoms, count):
    wide = inc_ref.shape[1]
    ids = lax.broadcasted_iota(jnp.int32, (8, atoms), 1)
    total = jnp.zeros((8, wide), f32)
    for steps in (ids % 4, ids // 4 % 4, ids // 16):
        part = dot((1.5 * steps.astype(f32)).astype(bf16), inc_ref[0:atoms, :])
        total = total + part * part
    lanes = lax.broadcasted_iota(jnp.int32, (8, wide), 1)
    padding = (lanes >= count).astype(f32)
    return lax.rsqrt(total + padding)[0:1, :], padding[0:1, :]


def loop(rows, block, body):
    block = min(rows, block)
    if rows == block:
        body(0, block)
        return

    def step(index, carry):
        body(pl.multiple_of(index * block, block), block)
        return carry

    lax.fori_loop(0, rows // block, step, 0)


def describe(split_ref, inc_ref, lat_ref, grad_ref, desc_ref, sq_ref):
    rows, wide = desc_ref.shape

    def body(start, block):
        lhs = split_ref[:, pl.ds(start, block), :].reshape(3 * block, -1)
        sq = jnp.zeros((block, 128), f32)
        for at in range(0, wide, CHUNK):
            cols = slice(at, at + CHUNK)
            off = dot(lhs, inc_ref[:, cols])
            off = [off[c * block : (c + 1) * block] for c in range(3)]
            inv = lax.rsqrt(
                off[0] * off[0] + off[1] * off[1] + off[2] * off[2] + lat_ref[1:2, cols]
            )
            desc = (inv - lat_ref[0:1, cols]).astype(bf16)
            desc_ref[pl.ds(start, block), cols] = desc
            cube = -(inv * inv * inv)
            for comp in range(3):
                grad_ref[comp, pl.ds(start, block), cols] = (off[comp] * cube).astype(grad_ref.dtype)
            wide_desc = desc.astype(f32)
            wide_desc = wide_desc * wide_desc
            for lane in range(0, CHUNK, 128):
                sq = sq + wide_desc[:, lane : lane + 128]
        sq_ref[pl.ds(start, block), :] = jnp.broadcast_to(
            jnp.sum(sq, axis=1, keepdims=True), (block, 128)
        )

    loop(rows, DESCRIBE_BLOCK, body)


def to_desc(split_ref, inc_ref, grad_ref, desc_ref, out_ref, self_ref):
    rows, wide = out_ref.shape

    def body(start, block):
        lhs = split_ref[:, pl.ds(start, block), :].reshape(3 * block, -1)
        total = jnp.zeros((block, 128), f32)
        for at in range(0, wide, CHUNK):
            cols = slice(at, at + CHUNK)
            diff = dot(lhs, inc_ref[:, cols])
            value = jnp.zeros((block, CHUNK), f32)
            for comp in range(3):
                grad = grad_ref[comp, pl.ds(start, block), cols].astype(f32)
                value = value + grad * diff[comp * block : (comp + 1) * block]
            value = value.astype(bf16)
            out_ref[pl.ds(start, block), cols] = value
            product = value.astype(f32) * desc_ref[pl.ds(start, block), cols].astype(f32)
            for lane in range(0, CHUNK, 128):
                total = total + product[:, lane : lane + 128]
        self_ref[pl.ds(start, block), :] = jnp.broadcast_to(
            jnp.sum(total, axis=1, keepdims=True), (block, 128)
        )

    loop(rows, DESC_BLOCK, body)


def mix_to_forces(diag_ref, vals_ref, cross_ref, desc_ref, own_ref, sum_ref, grad_ref, inc_t_ref, put):
    rows = own_ref.shape[0]
    wide = own_ref.shape[1]

    def body(start, block):
        diag = diag_ref[pl.ds(start, block), :]
        cross = cross_ref[pl.ds(start, block), :]
        sums = sum_ref[pl.ds(start, block), 0:1]
        forces = None
        for at in range(0, wide, CHUNK):
            cols = slice(at, at + CHUNK)
            value = dot(diag, vals_ref[:, cols]) + dot(cross, desc_ref[:, cols])
            value = value - own_ref[pl.ds(start, block), cols].astype(f32) * sums
            parts = []
            for comp in range(3):
                grad = grad_ref[comp, pl.ds(start, block), cols].astype(f32)
                parts.append((grad * value).astype(bf16))
            part = dot(jnp.concatenate(parts, axis=0), inc_t_ref[cols, :])
            forces = part if forces is None else forces + part
        put(start, block, [forces[c * block : (c + 1) * block] for c in range(3)])

    loop(rows, MIX_BLOCK, body)


def lane_sum(x):
    return jnp.broadcast_to(jnp.sum(x, axis=1, keepdims=True), (x.shape[0], 128))


def adjoint(ctx, put):
    rows = ctx.desc_t.shape[0]
    block = min(rows, 256)
    for at in range(0, rows, block):
        span = slice(at, at + block)
        project = dot(ctx.vals_t[span, :], ctx.desc_i[...], 1) - ctx.self_t[span, 0:1]
        product = (ctx.outer[span, :] * project).T
        ctx.cross_i[:, span] = product.astype(bf16)
        total = lane_sum(product)
        ctx.sum_i[...] = total if at == 0 else ctx.sum_i[...] + total
    mix_to_forces(
        ctx.diag_i, ctx.vals_t, ctx.cross_i, ctx.desc_t, ctx.desc_i, ctx.sum_i, ctx.grad_i, ctx.inc_t, put
    )


def forward(ctx, put):
    to_desc(ctx.vec_i, ctx.inc, ctx.grad_i, ctx.desc_i, ctx.vals_i, ctx.self_i)
    rows = ctx.desc_t.shape[0]
    block = min(rows, 256)
    self_row = ctx.self_i[...].T[0:1, :]
    for at in range(0, rows, block):
        span = slice(at, at + block)
        project = dot(ctx.desc_t[span, :], ctx.vals_i[...], 1) - self_row
        product = ctx.outer[span, :] * project
        ctx.cross_t[span, :] = product.astype(bf16)
        ctx.sum_t[span, :] = lane_sum(product)
    mix_to_forces(
        ctx.diag_t, ctx.vals_i, ctx.cross_t, ctx.desc_i, ctx.desc_t, ctx.sum_t, ctx.grad_t, ctx.inc_t, put
    )


def matern(ctx, length):
    rows = ctx.desc_t.shape[0]
    block = min(rows, 256)
    col_sq = ctx.self_i[...].T[0:1, :]
    for at in range(0, rows, block):
        span = slice(at, at + block)
        inner = dot(ctx.desc_t[span, :], ctx.desc_i[...], 1)
        square = ctx.sq_t[span, 0:1] + col_sq - 2.0 * inner
        radius = root_five * (jnp.sqrt(jnp.maximum(square, 0.0)) / length)
        falloff = jnp.exp(-radius)
        diag = 5.0 / (3.0 * length**2) * (1.0 + radius) * falloff
        ctx.diag_t[span, :] = diag.astype(bf16)
        ctx.diag_i[:, span] = diag.T.astype(bf16)
        ctx.outer[span, :] = 25.0 / (3.0 * length**4) * falloff


class Ctx:
    def __init__(self, names, refs):
        for name, ref in zip(names, refs):
            setattr(self, name, ref)


def scratch_of(rows_t, rows_i, wide, atoms, names):
    kinds = dict(
        inc=((3 * atoms, wide), bf16),
        inc_t=((wide, atoms), bf16),
        lat=((8, wide), f32),
        vec_t=((3, rows_t, 3 * atoms), bf16),
        vec_i=((3, rows_i, 3 * atoms), bf16),
        vals_t=((rows_t, wide), bf16),
        vals_i=((rows_i, wide), bf16),
        self_t=((rows_t, 128), f32),
        self_i=((rows_i, 128), f32),
        sum_t=((rows_t, 128), f32),
        sum_i=((rows_i, 128), f32),
        cross_t=((rows_t, rows_i), bf16),
        cross_i=((rows_i, rows_t), bf16),
    )
    return [pltpu.VMEM(*kinds[name]) for name in names]


def join_kernel(coords, forces, turned, pairs, both_out, turned_out, pairs_out, left, right, sems):
    width = coords.shape[1]
    copies = [
        pltpu.make_async_copy(source, target, sems.at[index])
        for index, (source, target) in enumerate(
            ((coords, left), (forces, right), (turned, turned_out), (pairs, pairs_out))
        )
    ]
    for copy in copies:
        copy.start()
    for copy in copies:
        copy.wait()
    both_out[:, :width] = left[...]
    both_out[:, width:] = right[...]


def train_kernel(n_train, atoms, out_names, *refs):
    both_t = refs[:n_train]
    pairs = refs[n_train]
    ctx = Ctx(out_names + ["vec_t"], refs[n_train + 1 :])
    build_incidence(pairs, ctx.inc, ctx.inc_t)
    lattice, padding = lattice_inverse(ctx.inc, atoms, pairs.shape[1])
    ctx.lat[0:1, :] = lattice
    ctx.lat[1:2, :] = padding
    rows = both_t[0].shape[0]
    for index, ref in enumerate(both_t):
        put_split(ctx.vec_t, index * rows, ref[:, : 3 * atoms], atoms)
    describe(ctx.vec_t, ctx.inc, ctx.lat, ctx.grad_t, ctx.desc_t, ctx.sq_t)
    for index, ref in enumerate(both_t):
        put_split(ctx.vec_t, index * rows, ref[:, 3 * atoms :], atoms)
    to_desc(ctx.vec_t, ctx.inc, ctx.grad_t, ctx.desc_t, ctx.vals_t, ctx.self_t)


def first_kernel(n_induce, atoms, in_names, out_names, scratch_names, *refs):
    coords_i = refs[:n_induce]
    length_ref = refs[n_induce]
    n_in = n_induce + 1 + len(in_names)
    partial, start_out = refs[n_in : n_in + 2]
    ctx = Ctx(in_names + out_names + scratch_names, refs[n_induce + 1 : n_in] + refs[n_in + 2 :])
    rows = coords_i[0].shape[1]
    for index, ref in enumerate(coords_i):
        put_split(ctx.vec_i, index * rows, ref[...].T, atoms)
    describe(ctx.vec_i, ctx.inc, ctx.lat, ctx.grad_i, ctx.desc_i, ctx.self_i)
    matern(ctx, length_ref[0])

    def put_start(start, block, parts):
        for comp in range(3):
            start_out[pl.ds(start, block), comp * atoms : (comp + 1) * atoms] = parts[comp]
            ctx.vec_i[comp, pl.ds(start, block), :] = split_three(parts[comp])

    adjoint(ctx, put_start)

    def put_partial(start, block, parts):
        for comp in range(3):
            partial[pl.ds(start, block), comp * atoms : (comp + 1) * atoms] = parts[comp]

    forward(ctx, put_partial)


def second_kernel(n_sum, n_train, atoms, in_names, scratch_names, *refs):
    parts_in = refs[:n_sum]
    both_t = refs[n_sum : n_sum + n_train]
    rest = refs[n_sum + n_train :]
    start_in = rest[0]
    n_in = len(in_names)
    ctx = Ctx(in_names, rest[1 : 1 + n_in])
    partial, coeffs_out, resid_out = rest[1 + n_in : 4 + n_in]
    for name, ref in zip(scratch_names, rest[4 + n_in :]):
        setattr(ctx, name, ref)
    rows = both_t[0].shape[0]
    probed_sq = jnp.zeros((1, 1), f32)
    cross_sq = jnp.zeros((1, 1), f32)
    for index in range(n_train):
        span = slice(index * rows, (index + 1) * rows)
        probed = parts_in[0][span, :]
        for ref in parts_in[1:]:
            probed = probed + ref[span, :]
        put_split(ctx.vec_t, index * rows, probed, atoms)
        probed_sq = probed_sq + jnp.sum(probed * probed, keepdims=True)
        cross_sq = cross_sq + jnp.sum(both_t[index][:, 3 * atoms :] * probed, keepdims=True)
    quotient = probed_sq / cross_sq
    center = 0.775 * quotient
    spread = 0.725 * quotient
    momentum = spread / center
    momentum_next = 1.0 / (2.0 * center / spread - momentum)

    def put_resid(start, block, parts):
        for comp in range(3):
            cols = slice(comp * atoms, (comp + 1) * atoms)
            first = start_in[pl.ds(start, block), cols]
            resid = first - parts[comp] / center
            direction = first / center
            coeffs = direction
            direction = momentum_next * momentum * direction + 2.0 * momentum_next / spread * resid
            resid_out[pl.ds(start, block), cols] = resid
            coeffs_out[pl.ds(start, block), cols] = coeffs + direction
            ctx.vec_i[comp, pl.ds(start, block), :] = split_three(direction)

    to_desc(ctx.vec_t, ctx.inc, ctx.grad_t, ctx.desc_t, ctx.vals_t, ctx.self_t)
    adjoint(ctx, put_resid)

    def put_partial(start, block, parts):
        for comp in range(3):
            partial[pl.ds(start, block), comp * atoms : (comp + 1) * atoms] = parts[comp]

    forward(ctx, put_partial)


def desc_kernel(atoms, coeffs, inc, grad_i, coeffs_out, out, vec):
    count, rows = out.shape
    own = coeffs[0:rows, :]
    put_split(vec, 0, own, atoms)
    coeffs_out[...] = own.T
    lhs = vec[...].reshape(3 * rows, -1)
    for at in range(0, inc.shape[1], CHUNK):
        end = min(at + CHUNK, count)
        diff = dot(lhs, inc[:, at : at + CHUNK])
        value = jnp.zeros((rows, CHUNK), f32)
        for comp in range(3):
            grad = grad_i[comp, 0:rows, at : at + CHUNK].astype(f32)
            value = value + grad * diff[comp * rows : (comp + 1) * rows]
        out[at:end, :] = value.T[: end - at, :]


def third_kernel(n_sum, atoms, in_names, scratch_names, *refs):
    parts_in = refs[:n_sum]
    resid_in = refs[n_sum]
    n_in = len(in_names)
    rest = refs[n_sum + 1 :]
    ctx = Ctx(in_names, rest[:n_in])
    resid_out = rest[n_in]
    for name, ref in zip(scratch_names, rest[n_in + 1 :]):
        setattr(ctx, name, ref)
    own = resid_out.shape[1]
    ctx.grad_i = ctx.grad_i.at[:, 0:own, :]
    ctx.desc_i = ctx.desc_i.at[0:own, :]
    ctx.diag_i = ctx.diag_i.at[0:own, :]
    ctx.outer = ctx.outer.at[:, 0:own]
    total = parts_in[0][...]
    for ref in parts_in[1:]:
        total = total + ref[...]
    put_split(ctx.vec_t, 0, total, atoms)

    def put_resid(start, block, parts):
        for comp in range(3):
            span = slice(comp * atoms, (comp + 1) * atoms)
            resid = resid_in[pl.ds(start, block), span] - parts[comp]
            resid_out[span, pl.ds(start, block)] = resid.T

    to_desc(ctx.vec_t, ctx.inc, ctx.grad_t, ctx.desc_t, ctx.vals_t, ctx.self_t)
    adjoint(ctx, put_resid)


def call(body, limit, ins, outs, scratch, fetch=False):
    vmem = pl.BlockSpec(memory_space=pltpu.VMEM)
    smem = pl.BlockSpec(memory_space=pltpu.SMEM)
    hbm = pl.BlockSpec(memory_space=pltpu.HBM)
    return pl.pallas_call(
        body,
        in_specs=[hbm if fetch else smem if x.ndim == 1 else vmem for x in ins],
        out_specs=[vmem for _ in outs],
        out_shape=outs,
        scratch_shapes=scratch,
        compiler_params=pltpu.CompilerParams(vmem_limit_bytes=limit),
    )(*ins)


def gather_rows(x, axis, size):
    others = [
        lax.ppermute(x, axis, [(i, i ^ step) for i in range(size)]) for step in range(1, size)
    ]
    return [x] + others


def per_device(n_train, n_induce, train_coords, induce_coords, train_forces, atom_pairs, length_scale):
    atoms = train_coords.shape[1] // 3
    count = atom_pairs.shape[1]
    wide = -(-count // CHUNK) * CHUNK
    gather = math.gcd(GATHER, n_induce // 2)
    rows_t = n_train * train_coords.shape[0]
    own = induce_coords.shape[0]
    rows_i = gather * own
    grad_dtype = f32 if (rows_t + rows_i) * wide * 12 <= 20 * MIB else bf16
    kinds = dict(
        grad_t=((3, rows_t, wide), grad_dtype),
        grad_i=((3, rows_i, wide), grad_dtype),
        desc_t=((rows_t, wide), bf16),
        desc_i=((rows_i, wide), bf16),
        diag_t=((rows_t, rows_i), bf16),
        diag_i=((rows_i, rows_t), bf16),
        outer=((rows_t, rows_i), f32),
        inc=((3 * atoms, wide), bf16),
        inc_t=((wide, atoms), bf16),
        lat=((8, wide), f32),
        vals_t=((rows_t, wide), bf16),
        sq_t=((rows_t, 128), f32),
        self_t=((rows_t, 128), f32),
    )
    size = sum(math.prod(shape) * jnp.dtype(dtype).itemsize for shape, dtype in kinds.values())
    stays = size <= 32 * MIB and rows_t <= 256
    limit = 24 * MIB if stays else 60 * MIB
    sds = jax.ShapeDtypeStruct
    kept = pltpu.VMEM if stays else sds

    def pin(xs):
        return [pltpu.with_memory_space_constraint(x, pltpu.VMEM) for x in xs] if stays else xs

    fetched = [train_coords, train_forces, induce_coords.T, atom_pairs]
    both, turned, pairs = call(
        join_kernel,
        limit,
        [pltpu.with_memory_space_constraint(x, pltpu.HBM) for x in fetched],
        [kept((train_coords.shape[0], 6 * atoms), f32), kept((3 * atoms, own), f32), kept(atom_pairs.shape, atom_pairs.dtype)],
        [pltpu.VMEM(train_coords.shape, f32)] * 2 + [pltpu.SemaphoreType.DMA((4,))],
        fetch=True,
    )
    both_t = gather_rows(both, "train", n_train)
    coords_i = [turned] + [
        lax.ppermute(turned, "induce", [(i, i ^ (2 * step)) for i in range(n_induce)])
        for step in range(1, gather)
    ]
    both_t = both_t[:1] + pin(both_t[1:])
    coords_i = coords_i[:1] + pin(coords_i[1:])

    train_names = ["grad_t", "desc_t", "inc", "inc_t", "lat", "vals_t", "sq_t", "self_t"]
    train_state = call(
        functools.partial(train_kernel, n_train, atoms, train_names),
        limit,
        both_t + [pairs],
        [kept(*kinds[name]) for name in train_names],
        scratch_of(rows_t, rows_i, wide, atoms, ["vec_t"]),
    )
    induce_names = ["grad_i", "desc_i", "diag_t", "diag_i", "outer"]
    names = ["vec_i", "vals_i", "self_i", "sum_t", "sum_i", "cross_t", "cross_i"]
    vec_t = sds((rows_t, 3 * atoms), f32)
    vec_i = sds((rows_i, 3 * atoms), f32)
    partial, start, *induce_state = call(
        functools.partial(first_kernel, gather, atoms, train_names, induce_names, names),
        limit,
        coords_i + [length_scale] + list(train_state),
        [vec_t, vec_i] + [kept(*kinds[name]) for name in induce_names],
        scratch_of(rows_t, rows_i, wide, atoms, names),
    )
    kept_names = ["grad_t", "desc_t", "inc", "inc_t"] + induce_names
    state = list(train_state[:4]) + list(induce_state)

    def reduce_parts(x):
        step = 2 * gather
        while step < n_induce:
            x = x + lax.ppermute(x, "induce", [(i, i ^ step) for i in range(n_induce)])
            step *= 2
        return pin([x, lax.ppermute(x, "induce", [(i, i ^ 1) for i in range(n_induce)])])

    names = ["vec_t", "vals_t", "self_t"] + names
    parts = reduce_parts(partial)
    partial, coeffs, resid = call(
        functools.partial(second_kernel, len(parts), n_train, atoms, kept_names, names),
        limit,
        parts + both_t + [start] + state,
        [vec_t, vec_i, vec_i],
        scratch_of(rows_t, rows_i, wide, atoms, names),
    )
    parts = reduce_parts(partial)
    own_vec = sds((3 * atoms, own), f32)
    coeffs, desc_coeffs = call(
        functools.partial(desc_kernel, atoms),
        limit,
        [coeffs, state[2], state[4]],
        [own_vec, sds((count, own), f32)],
        scratch_of(rows_t, own, wide, atoms, ["vec_i"]),
    )
    names = ["vec_t", "vals_t", "self_t", "sum_i", "cross_i"]
    in_names = kept_names
    (resid,) = call(
        functools.partial(third_kernel, len(parts), atoms, in_names, names),
        limit,
        parts + [resid] + state,
        [own_vec],
        scratch_of(rows_t, own, wide, atoms, names),
    )
    return (coeffs.T, resid.T, desc_coeffs.T)


def solution(mesh):
    in_specs = (P("train", None), P("induce", None), P("train", None), P(), P())
    out_specs = (P("induce", None), P("induce", None), P("induce", None))
    body = functools.partial(per_device, mesh.shape["train"], mesh.shape["induce"])
    return jax.shard_map(
        body, mesh=mesh, in_specs=in_specs, out_specs=out_specs, check_vma=False
    )
```
